512 devices in a mesh: parts: 2 (over y), seq: 32 (over z), tp: 8 (over x, core).
Axes of the slice: x: 4, y: 2, z: 32, core: 2. Of those that a mesh axis runs over, the one named last changes fastest.
The devices are a block of a 4x8x32 slice.
Arguments:
- tokens: bfloat16 [16384, 8192], P(('parts', 'seq'), 'tp'), parts along dimension 0, may hold values from -6 to 6
- norm_gain: bfloat16 [8192], P('tp'), may hold values from 0.099609375 to 1.8984375
- w_query: bfloat16 [8192, 4096], P('seq', 'tp'), may hold values from -0.0625 to 0.0625
- w_kv: bfloat16 [8192, 2, 1024], P('seq', None, 'tp'), may hold values from -0.0625 to 0.0625
- b_query: float32 [4096], P('tp'), may hold values from -4 to 4
- b_kv: float32 [2, 1024], P(None, 'tp'), may hold values from -4 to 4
- kv_pool: bfloat16 [8192, 2, 8, 1024], P(('parts', 'seq'), None, None, 'tp'), parts along dimension 0, may hold values from -68 to 68
- prefix_pages: int32 [128, 32], P('parts'), parts along dimension 0, may hold values from 0 to 4095, as said below
- prefix_len: int32 [128], P('parts'), parts along dimension 0, may hold values from 0 to 256
- suffix_len: int32 [128], P('parts'), parts along dimension 0, may hold values from 1 to 128
- fresh_owner: int32 [2048, 1], P('parts'), parts along dimension 0, may hold values from 0 to 31; in each aligned block of 32 rows (0 to 31, 32 to 63, ...) at most 2 rows name the same one
Outputs:
- attn_out: bfloat16 [16384, 4096], P(('parts', 'seq'), 'tp'), parts along dimension 0
- fresh_pages: bfloat16 [4096, 2, 8, 1024], P(('parts', 'seq'), None, None, 'tp'), parts along dimension 0
The draws below stay inside these ranges and needn't reach their ends.
There are 2 independent parts, one for each index of `parts`. The reference program is written for one: setup_inputs(seed, part) draws one part's arguments, and reference() takes and returns one part's arrays. A program takes and returns all parts, laid end to end along the dimension named above; an argument that names none is the same for every part. Nothing has to cross between parts.
Inputs may be any that keep to these rules, and one draw needn't show every extreme that they name: `prefix_pages`: page id q lies in the 128 pages of sequence group q // 128. Among the 64 entries of requests 2*g to 2*(g+1)-1, no group holds more than 3, and in every such block some group holds exactly 3. Entries past the matched prefix still name pages. `fresh_owner`: in the rows of one sequence group's requests (aligned blocks of 32 rows) no group is named more than 2 times; some blocks name one exactly 2 times.
All inputs are finite; a program needn't handle non-finite values.
Results may differ from the reference program's by a relative error of at most 0.005.
The reference program's roundings to bfloat16 on the way (of `normed` and `probs`) count: a program that leaves them out, or rounds other values in their place, can miss the bound.
Values may be sent and summed in bfloat16 or wider, within the bound.
A program may use at most 64 MiB of HBM per device.

```python
import math
import jax
import jax.numpy as jnp
import numpy as np
from jax import lax

D = 8192
HEADS = 32
KV_HEADS = 8
HEAD_DIM = 128
BLOCK = 128
PAGE = 8
PMAX = 32
BLK_DEV = 2
PAGES_DEV = 128
REQS = 64
TOKENS = 8192
SUF_PAGES = 16
POOL = 4096
C_PRE = 3
C_NEW = 2
FRESH = 2048
N_SEQ = 32


def draw_prefix_pages(key, part):
    entries = BLK_DEV * PMAX
    items = C_PRE * N_SEQ

    def one_block(block_key):
        first_key, second_key, third_key, fourth_key = jax.random.split(block_key, 4)
        order = jax.random.permutation(first_key, N_SEQ).astype(jnp.int32)
        item_ids = jnp.arange(items, dtype=jnp.int32)
        owner_of = order[item_ids % N_SEQ]
        scores = jax.random.randint(second_key, (items,), 1, 1 << 20, dtype=jnp.int32)
        scores = jnp.where(item_ids % N_SEQ == 0, 0, scores)
        picked = jnp.argsort(scores * items + item_ids, stable=True)[:entries]
        owners = owner_of[picked]
        owners = owners[jax.random.permutation(third_key, entries)]
        slots = jax.random.randint(fourth_key, (entries,), 0, PAGES_DEV, dtype=jnp.int32)
        return (owners * PAGES_DEV + slots).astype(jnp.int32)
    block_keys = jax.random.split(jax.random.fold_in(key, 11), N_SEQ)
    return jax.vmap(one_block)(block_keys).reshape(REQS, PMAX)


def draw_kv_pool(key, part):
    shape = (POOL, 2, PAGE, KV_HEADS * HEAD_DIM)
    first_key = jax.random.fold_in(jax.random.fold_in(key, 23), 0)
    return jnp.clip(jax.random.normal(first_key, shape, jnp.float32), -6.0, 6.0).astype(jnp.bfloat16)


def set_ends(values, rng, low, high):
    place = [jax.random.randint(jax.random.fold_in(rng, axis), (), 0, length) for axis, length in enumerate(values.shape)]
    widest = values.shape.index(max(values.shape))
    beside = place[:widest] + [(place[widest] + 1) % values.shape[widest]] + place[widest + 1:]
    return values.at[tuple(place)].set(low).at[tuple(beside)].set(high)


def shard_levels(rng, shape, cuts, smallest, top_value):
    loudness = 1.0
    for dim, blocks in cuts:
        steps = jax.random.uniform(jax.random.fold_in(jax.random.fold_in(rng, 6), dim), (blocks,), jnp.float32, smallest / len(cuts), top_value / len(cuts))
        loudness = loudness * jnp.repeat(jnp.exp(steps), shape[dim] // blocks).reshape((-1,) + (1,) * (len(shape) - 1 - dim))
    return loudness


def deal_out(stream_key, own, number, rows, count, top, bound, lean):
    order = jax.random.permutation(stream_key, count)
    crowded, usual = load_shares(count, rows * top, bound, lean, True), load_shares(count, rows * top, bound, lean, False)
    places = jnp.arange(count)

    def named(tallies, turn):
        used = int((tallies > 0).sum())
        fixed = max(1, used // 4)
        passed = fixed + (places - fixed + turn * (used - fixed)) % max(1, count - fixed)
        return jnp.zeros((count,), jnp.int32).at[order[jnp.where(places < fixed, places, passed)]].set(jnp.asarray(tallies, jnp.int32))

    tallies = jnp.where(number % 4 == 0, named(crowded, number // 4), named(usual, number - number // 4 - 1))
    mixed = jax.random.permutation(jax.random.fold_in(own, 3), count)
    giver, receiver = mixed[0:count // 2 * 2:2], mixed[1:count // 2 * 2:2]
    slack = jnp.minimum(tallies[giver] - 1, bound - tallies[receiver]) // 2
    slack = jnp.where((giver == order[0]) | (receiver == order[0]) | (tallies[receiver] == 0), 0, jnp.maximum(slack, 0))
    passed = jax.random.randint(jax.random.fold_in(own, 4), (count // 2,), 0, 1 << 20) % (slack + 1)
    tallies = tallies.at[giver].add(-passed).at[receiver].add(passed)
    labels = jnp.searchsorted(jnp.cumsum(tallies), jnp.arange(rows * top), side="right").astype(jnp.int32)
    grid = labels.reshape(top, rows).T
    grid = grid[jax.random.permutation(jax.random.fold_in(own, 1), rows)]
    turn = jax.random.randint(jax.random.fold_in(own, 2), (rows, 1), 0, top)
    return jnp.take_along_axis(grid, (jnp.arange(top)[None, :] + turn) % top, axis=1)


def load_shares(amount, total, bound, slope, full):
    portions = [(1 << 20) // math.isqrt(standing ** slope) + 1 for standing in range(1, amount + 1)]
    largest = bound if full else min(bound, max(-(-total // amount), total * portions[0] // sum(portions)))
    least = 1 if total - largest >= amount - 1 else 0
    holding, spare = [largest] + [least] * (amount - 1), total - largest - least * (amount - 1)
    while spare > 0:
        free = [i for i in range(1, amount) if holding[i] < largest] or [i for i in range(1, amount) if holding[i] < bound]
        whole, left = sum([portions[i] for i in free]), spare
        for i in free:
            more = min(bound - holding[i], max(1, left * portions[i] // whole), spare)
            holding[i] = holding[i] + more
            spare = spare - more
    return np.array(holding)


def normal_values(stream_key, dims, deviation, reach, pieces=(), kind=jnp.bfloat16):
    loudness = shard_levels(stream_key, dims, pieces, -0.22, 0.18) if pieces else 1.0
    result = jax.random.normal(stream_key, dims, jnp.float32) * deviation * loudness
    return jnp.minimum(jnp.maximum(result, -reach), reach).astype(kind)


def setup_inputs(seed: int = 0, part: int = 0) -> dict:
    key_list = jax.random.split(jax.random.key(seed), 12)
    own_keys = jax.random.split(jax.random.fold_in(key_list[11], part), 12)
    tokens = normal_values(own_keys[0], (TOKENS, D), 1.0, 6.0, ((0, 32), (1, 8)))
    norm_gain = jnp.clip(1.0 + 0.18 * jax.random.normal(key_list[1], (D,), jnp.float32), 0.099609375, 1.8984375).astype(jnp.bfloat16)
    w_query = normal_values(key_list[2], (D, HEADS * HEAD_DIM), D ** -0.5, 0.0625, ((0, 32), (1, 8)))
    w_kv = normal_values(key_list[3], (D, 2, KV_HEADS * HEAD_DIM), D ** -0.5, 0.0625, ((0, 32), (2, 8)))
    b_query = normal_values(key_list[4], (HEADS * HEAD_DIM,), 1.0, 4.0, ((0, 8),), jnp.float32)
    b_kv = normal_values(key_list[5], (2, KV_HEADS * HEAD_DIM), 1.0, 4.0, ((1, 8),), jnp.float32)
    kv_pool = draw_kv_pool(jax.random.fold_in(jax.random.fold_in(key_list[11], part), 71), part)
    prefix_pages = draw_prefix_pages(jax.random.fold_in(jax.random.fold_in(key_list[11], part), 71), part)
    prefix_len = set_ends(jax.random.randint(own_keys[8], (REQS,), 0, PMAX * PAGE + 1), jax.random.fold_in(own_keys[8], 1), 0, PMAX * PAGE).astype(jnp.int32)
    suffix_len = set_ends(jax.random.randint(own_keys[9], (REQS,), 1, BLOCK + 1), jax.random.fold_in(own_keys[9], 1), 1, BLOCK).astype(jnp.int32)
    fresh_owner_keys = jax.random.split(jax.random.fold_in(own_keys[10], 1), (REQS * SUF_PAGES) // (BLK_DEV * SUF_PAGES))
    fresh_owner_turns = jax.random.permutation(jax.random.fold_in(own_keys[10], 3), (REQS * SUF_PAGES) // (BLK_DEV * SUF_PAGES))
    fresh_owner = jax.vmap(lambda own, number: deal_out(jax.random.fold_in(own_keys[10], 2), own, number, BLK_DEV * SUF_PAGES, N_SEQ, 1, C_NEW, 2))(fresh_owner_keys, fresh_owner_turns).reshape((REQS * SUF_PAGES, 1))
    return {"tokens": tokens, "norm_gain": norm_gain, "w_query": w_query, "w_kv": w_kv, "b_query": b_query, "b_kv": b_kv, "kv_pool": kv_pool, "prefix_pages": prefix_pages, "prefix_len": prefix_len, "suffix_len": suffix_len, "fresh_owner": fresh_owner}


def rotate(values, positions):
    half_dim = values.shape[-1] // 2
    freq_index = jnp.arange(half_dim, dtype=jnp.float32)
    inverse = jnp.exp(freq_index * (-2.0 * math.log(1000000.0) / values.shape[-1]))
    angles = positions.astype(jnp.float32)[..., None, None] * inverse
    cosine = jnp.cos(angles)
    sine = jnp.sin(angles)
    first_half = values[..., :half_dim]
    second_half = values[..., half_dim:]
    return jnp.concatenate([first_half * cosine - second_half * sine, second_half * cosine + first_half * sine], axis=-1)

def attend(query, key_new, value_new, key_old, value_old, prefix_mine, suffix_mine):
    batch, block_len, heads_here, head_dim = query.shape
    kv_here = key_new.shape[2]
    group_size = heads_here // kv_here
    old_len = key_old.shape[1]
    grouped = query.reshape(batch, block_len, kv_here, group_size, head_dim)
    all_keys = jnp.concatenate([key_old, key_new], axis=1)
    all_values = jnp.concatenate([value_old, value_new], axis=1)
    scores = jnp.einsum('btkgd,bskd->bkgts', grouped.astype(jnp.float32), all_keys.astype(jnp.float32)) / math.sqrt(head_dim)
    key_pos = jnp.arange(old_len + block_len, dtype=jnp.int32)
    query_pos = jnp.arange(block_len, dtype=jnp.int32)
    in_prefix = key_pos[None, None, :] < prefix_mine[:, None, None]
    shifted = key_pos - old_len
    in_suffix = (shifted[None, None, :] <= query_pos[None, :, None]) & (shifted[None, None, :] < suffix_mine[:, None, None])
    allowed = jnp.where(key_pos[None, None, :] < old_len, in_prefix, in_suffix)[:, None, None]
    masked = jnp.where(allowed, scores, -1e+30)
    peak = lax.optimization_barrier(jnp.max(masked, axis=-1, keepdims=True))
    weights = jnp.where(allowed, jnp.exp(masked - peak), 0.0)
    probs = (weights / lax.optimization_barrier(jnp.sum(weights, axis=-1, keepdims=True))).astype(jnp.bfloat16)
    mixed = jnp.einsum('bkgts,bskd->btkgd', probs.astype(jnp.float32), all_values.astype(jnp.float32))
    live = query_pos[None, :] < suffix_mine[:, None]
    mixed = jnp.where(live[:, :, None, None, None], mixed, 0.0)
    return mixed.reshape(batch * block_len, heads_here * head_dim).astype(jnp.bfloat16)

def reference(tokens, norm_gain, w_query, w_kv, b_query, b_kv, kv_pool, prefix_pages, prefix_len, suffix_len, fresh_owner):
    kv_width = KV_HEADS * HEAD_DIM
    widened = tokens.astype(jnp.float32)
    mean_square = lax.optimization_barrier(jnp.mean(widened * widened, axis=-1, keepdims=True))
    normed = (widened * lax.rsqrt(mean_square + 1e-06) * norm_gain.astype(jnp.float32)).astype(jnp.bfloat16)
    query_lin = jnp.dot(normed, w_query, preferred_element_type=jnp.float32) + b_query
    pair_lin = jnp.dot(normed, w_kv.reshape(D, 2 * kv_width), preferred_element_type=jnp.float32) + b_kv.reshape(2 * kv_width)
    slot_ids = jnp.arange(BLOCK, dtype=jnp.int32)
    positions = prefix_len[:, None] + slot_ids[None, :]
    live = (slot_ids[None, :] < suffix_len[:, None])[:, :, None, None]
    query = rotate(query_lin.reshape(REQS, BLOCK, HEADS, HEAD_DIM), positions).astype(jnp.bfloat16)
    key_new = jnp.where(live, rotate(pair_lin[:, :kv_width].reshape(REQS, BLOCK, KV_HEADS, HEAD_DIM), positions), 0.0).astype(jnp.bfloat16)
    value_new = jnp.where(live, pair_lin[:, kv_width:].reshape(REQS, BLOCK, KV_HEADS, HEAD_DIM), 0.0).astype(jnp.bfloat16)

    def one_request(packed):
        query_one, key_one, value_one, page_row, prefix_one, suffix_one = packed
        pages = kv_pool[page_row]
        key_old = pages[:, 0].reshape(1, PMAX * PAGE, KV_HEADS, HEAD_DIM)
        value_old = pages[:, 1].reshape(1, PMAX * PAGE, KV_HEADS, HEAD_DIM)
        return attend(query_one[None], key_one[None], value_one[None], key_old, value_old, prefix_one[None], suffix_one[None])
    attn_out = lax.map(one_request, (query, key_new, value_new, prefix_pages, prefix_len, suffix_len))
    attn_out = attn_out.reshape(TOKENS, HEADS * HEAD_DIM)
    new_pages = jnp.stack([key_new.reshape(REQS * SUF_PAGES, PAGE, kv_width), value_new.reshape(REQS * SUF_PAGES, PAGE, kv_width)], axis=1)
    owners = fresh_owner[:, 0].reshape(N_SEQ, BLK_DEV * SUF_PAGES)
    order_ids = jnp.arange(BLK_DEV * SUF_PAGES, dtype=jnp.int32)
    earlier = (owners[:, :, None] == owners[:, None, :]) & (order_ids[None, None, :] < order_ids[None, :, None])
    ranks = lax.optimization_barrier(jnp.sum(earlier.astype(jnp.int32), axis=-1))
    groups = jnp.arange(N_SEQ, dtype=jnp.int32)[:, None]
    target = ((owners * N_SEQ + groups) * C_NEW + ranks).reshape(-1).astype(jnp.int32)
    fresh_pages = jnp.zeros((FRESH, 2, PAGE, kv_width), jnp.bfloat16).at[target].set(new_pages)
    return (attn_out, fresh_pages)
```

```python
import functools
import math

import jax
import jax.numpy as jnp
from jax import lax
from jax.experimental import pallas as pl
from jax.experimental.pallas import tpu as pltpu
from jax.sharding import PartitionSpec as P

HEAD_DIM = 128
BLOCK = 128
PAGE = 8
MESH = pl.DeviceIdType.MESH

NORM_AT = 7
PREFIX_LAG = 12
CATCH_UP = 4


def offsets(count):
    starts, at = [], 0
    for step in range(1, count + 1):
        starts.append(at)
        at += count - step + 1
    return starts, at


class Ring:
    def __init__(self, make, steps):
        self.make, self.steps, self.started = make, steps, {}

    def start(self, step):
        if step > self.steps:
            return
        if step > 2:
            self.started.pop(step - 2).wait_send()
        copy = self.make(step)
        copy.start()
        self.started[step] = copy

    def arrive(self, step):
        if step <= self.steps:
            self.make(step).wait_recv()

    def drain(self):
        for copy in self.started.values():
            copy.wait_send()
        self.started = {}


def gather_kernel(
    n_parts, n_seq, n_tp,
    tok_ref, gain_ref, wkv_ref, wq_ref, bkv_ref, cos_ref, sin_ref, live_ref, psend_ref, source_ref,
    q0_ref, q1_ref, knew_ref, vnew_ref, got_ref, fresh_ref,
    toks, gains, nrm, wkvb, wqb0, wqb1, acc, pg_r, pg_l, fsend, fg_r, fg_l, newp,
    ring_send, ring_recv, y_send, y_recv, tok_send, tok_recv, gain_send, gain_recv,
):
    part, me, tp = lax.axis_index("parts"), lax.axis_index("seq"), lax.axis_index("tp")
    right, left = lax.rem(me + 1, n_seq), lax.rem(me + n_seq - 1, n_seq)
    up, down = lax.rem(part + 1, n_parts), lax.rem(part + n_parts - 1, n_parts)
    n_r, n_l = n_seq // 2, (n_seq - 1) // 2
    y_r, y_l = n_parts // 2, (n_parts - 1) // 2
    partner = tp + 1 - 2 * lax.rem(tp, 2)
    x_right, x_left = lax.rem(tp + 2, n_tp), lax.rem(tp + n_tp - 2, n_tp)
    x_far = lax.rem(tp + n_tp // 2, n_tp)
    rows = tok_ref.shape[0]
    half = rows // 2
    depth = wkv_ref.shape[0]
    features = tok_ref.shape[1]

    barrier = pltpu.get_barrier_semaphore()
    greeted = [{"seq": right}, {"seq": left}]
    greeted += [{"tp": lax.rem(tp + r, n_tp)} for r in range(1, n_tp)]
    if n_parts > 1:
        greeted.append({"parts": up})
    if n_parts > 2:
        greeted.append({"parts": down})
    for device in greeted:
        pl.semaphore_signal(barrier, inc=1, device_id=device, device_id_type=MESH)
    pl.semaphore_wait(barrier, len(greeted))

    def remote(src, dst, send, recv, device):
        return pltpu.make_async_remote_copy(
            src_ref=src, dst_ref=dst, send_sem=send, recv_sem=recv,
            device_id=device, device_id_type=MESH,
        )

    def slot(direction, step):
        return 2 * step - 1 if direction == 0 else 2 * step

    def ring(stream, direction, make_refs):
        target = {"seq": right if direction == 0 else left}

        def make(step):
            src, dst = make_refs(step)
            return remote(
                src, dst, ring_send.at[stream, direction, step % 2],
                ring_recv.at[stream, direction, step - 1], target,
            )

        return Ring(make, n_r if direction == 0 else n_l)

    def kv_refs(direction):
        def refs(step):
            src = wkv_ref if step == 1 else wkvb.at[slot(direction, step - 1)]
            return src, wkvb.at[slot(direction, step)]

        return refs

    q_cols = q0_ref.shape[1]

    def q_refs(direction, buffer, which):
        def refs(step):
            if step == 1:
                src = wq_ref.at[part, :, pl.ds(which * q_cols, q_cols)]
            else:
                src = buffer.at[slot(direction, step - 1), part]
            return src, buffer.at[slot(direction, step), part]

        return refs

    starts_r, _ = offsets(n_r)
    starts_l, _ = offsets(n_l)

    def block_refs(direction, first, buffer):
        count = n_r if direction == 0 else n_l
        starts = starts_r if direction == 0 else starts_l

        def refs(step):
            size = count - step + 1
            if step == 1:
                src = first.at[pl.ds(1 if direction == 0 else 1 + n_r, count)]
            else:
                src = buffer.at[pl.ds(starts[step - 2] + 1, size)]
            return src, buffer.at[pl.ds(starts[step - 1], size)]

        return refs

    kv = [ring(0, d, kv_refs(d)) for d in (0, 1)]
    q_ring = [
        [ring(1 + w, d, q_refs(d, buffer, w)) for d in (0, 1)]
        for w, buffer in enumerate((wqb0, wqb1))
    ]
    prefix = [ring(3, d, block_refs(d, psend_ref, (pg_r, pg_l)[d])) for d in (0, 1)]
    fresh = [ring(4, d, block_refs(d, fsend, (fg_r, fg_l)[d])) for d in (0, 1)]

    y_open = {}

    def y_make(which, step, direction, hop):
        buffer = (wqb0, wqb1)[which]
        origin = lax.rem(part + (n_parts - hop + 1 if direction == 0 else hop - 1), n_parts)
        pair = pl.ds(2 * step - 1, 2 if step <= n_l else 1)
        lane = hop - 1 if direction == 0 else y_r + hop - 1
        return remote(
            buffer.at[pair, origin], buffer.at[pair, origin],
            y_send.at[which, lane, step % 2], y_recv.at[which, lane, step - 1],
            {"parts": up if direction == 0 else down},
        )

    def y_start(which, step, direction, hop):
        if hop > (y_r if direction == 0 else y_l):
            return
        key = (which, direction, hop)
        if (key, step - 2) in y_open:
            y_open.pop((key, step - 2)).wait_send()
        copy = y_make(which, step, direction, hop)
        copy.start()
        y_open[(key, step)] = copy

    def y_arrive(which, step, direction, hop):
        if hop > (y_r if direction == 0 else y_l):
            return
        buffer = (wqb0, wqb1)[which]
        origin = lax.rem(part + (n_parts - hop if direction == 0 else hop), n_parts)
        pair = pl.ds(2 * step - 1, 2 if step <= n_l else 1)
        lane = hop - 1 if direction == 0 else y_r + hop - 1
        remote(
            buffer.at[pair, origin], buffer.at[pair, origin],
            y_send.at[which, lane, step % 2], y_recv.at[which, lane, step - 1],
            {"parts": up if direction == 0 else down},
        ).wait_recv()

    lo, hi = pl.ds(0, half), pl.ds(half, half)

    def tok_copy(index, src, block, part_rows, device):
        dst = toks.at[block] if part_rows is None else toks.at[block, part_rows]
        if src is None:
            src = dst
        return remote(src, dst, tok_send.at[index], tok_recv.at[index], {"tp": device})

    tok_open = []

    def tok_start(*args):
        copy = tok_copy(*args)
        copy.start()
        tok_open.append(copy)

    for d in (0, 1):
        kv[d].start(1)
        q_ring[0][d].start(1)
    tok_start(1, tok_ref, tp, None, x_right)
    tok_start(2, tok_ref, tp, None, x_left)
    tok_start(0, tok_ref, tp, None, partner)
    gain_open = []
    for r in range(1, n_tp):
        copy = remote(
            gain_ref, gains.at[tp], gain_send.at[r - 1], gain_recv.at[r - 1],
            {"tp": lax.rem(tp + r, n_tp)},
        )
        copy.start()
        gain_open.append(copy)
    toks[tp] = tok_ref[...]
    gains[tp] = gain_ref[...]
    acc[...] = jnp.zeros_like(acc)
    q0_ref[...] = jnp.zeros_like(q0_ref)
    q1_ref[...] = jnp.zeros_like(q1_ref)
    got_ref[0] = psend_ref[0]

    def tokens_near():
        tok_copy(1, None, x_left, None, x_right).wait_recv()
        tok_start(5, None, x_left, lo, x_right)
        tok_start(3, None, x_left, None, partner)
        tok_copy(2, None, x_right, None, x_left).wait_recv()
        tok_start(6, None, x_right, hi, x_left)
        tok_start(4, None, x_right, None, partner)

    def tokens_far():
        tok_copy(5, None, x_far, lo, x_right).wait_recv()
        tok_start(7, None, x_far, lo, partner)
        tok_copy(6, None, x_far, hi, x_left).wait_recv()
        tok_start(8, None, x_far, hi, partner)

    def shifted(base, by):
        return lax.rem(base + by, n_tp)

    def normalise():
        p_left, p_right = shifted(partner, n_tp - 2), shifted(partner, 2)
        p_far = shifted(partner, n_tp // 2)
        for index, block, part_rows in (
            (0, partner, None), (3, p_left, None), (4, p_right, None),
            (7, p_far, lo), (8, p_far, hi),
        ):
            tok_copy(index, None, block, part_rows, partner).wait_recv()
        for r in range(1, n_tp):
            remote(
                gain_ref, gains.at[lax.rem(tp + n_tp - r, n_tp)],
                gain_send.at[r - 1], gain_recv.at[r - 1], {"tp": lax.rem(tp + r, n_tp)},
            ).wait_recv()
        step_rows = 16

        def some_rows(i, carry):
            at = pl.ds(pl.multiple_of(i * step_rows, step_rows), step_rows)
            total = jnp.zeros((step_rows, features), jnp.float32)
            for t in range(n_tp):
                wide = toks[t, at, :].astype(jnp.float32)
                total = total + wide * wide
            mean = jnp.sum(total, axis=1, keepdims=True) / (n_tp * features)
            scale = lax.rsqrt(mean + 1e-06)
            for t in range(n_tp):
                wide = toks[t, at, :].astype(jnp.float32)
                value = (wide * scale * gains[t]).astype(jnp.bfloat16)
                for j in range(features // depth):
                    nrm[t * (features // depth) + j, at, :] = value[:, j * depth : (j + 1) * depth]
            return carry

        lax.fori_loop(0, rows // step_rows, some_rows, 0)

    def origin(direction, step):
        return lax.rem(me + (n_seq - step if direction == 0 else step), n_seq)

    def dot(shard, weight):
        return jnp.dot(nrm[shard], weight, preferred_element_type=jnp.float32)

    def kv_product(step):
        if step == 0:
            acc[...] += dot(me, wkv_ref[...])
            return
        total = dot(origin(0, step), wkvb[2 * step - 1])
        if step <= n_l:
            total = total + dot(origin(1, step), wkvb[2 * step])
        acc[...] += total

    def q_product(which, step):
        out, buffer = ((q0_ref, wqb0), (q1_ref, wqb1))[which]
        if step == 0:
            own = wq_ref[:, :, which * q_cols : (which + 1) * q_cols]
            out[...] += dot(me, own.reshape(depth, q_cols))
            return
        total = dot(origin(0, step), buffer[2 * step - 1].reshape(depth, q_cols))
        if step <= n_l:
            total = total + dot(origin(1, step), buffer[2 * step].reshape(depth, q_cols))
        out[...] += total

    def finish_kv():
        pair = acc[...] + bkv_ref[...]
        key, value = pair[:, :HEAD_DIM], pair[:, HEAD_DIM:]
        turned = key * cos_ref[...] + pltpu.roll(key, HEAD_DIM // 2, 1) * sin_ref[...]
        key = turned * live_ref[...]
        value = value * live_ref[...]
        knew_ref[...] = key.astype(jnp.bfloat16)
        vnew_ref[...] = value.astype(jnp.bfloat16)
        pages = rows // PAGE
        newp[pl.ds(0, pages), 0] = key.reshape(pages, PAGE, HEAD_DIM).astype(jnp.bfloat16)
        newp[pl.ds(0, pages), 1] = value.reshape(pages, PAGE, HEAD_DIM).astype(jnp.bfloat16)
        newp[pages] = jnp.zeros((2, PAGE, HEAD_DIM), jnp.bfloat16)

        cap = fsend.shape[1]

        def select(i, carry):
            for c in range(cap):
                fsend[i, c] = newp[source_ref[i * cap + c]]
            return carry

        lax.fori_loop(0, n_seq, select, 0)
        fresh_ref[me] = fsend[0]

    pending = []
    y_max = max(y_r, y_l)
    fresh_from = n_r + 1
    last = max(2 * n_r + 1 + y_max, n_r + PREFIX_LAG, fresh_from + n_r)
    for it in range(1, last + 1):
        for d in (0, 1):
            if it <= n_r:
                kv[d].arrive(it)
                kv[d].start(it + 1)
        for w in (0, 1):
            step = it - w * n_r
            if w == 1 and step == 0:
                for d in (0, 1):
                    q_ring[1][d].start(1)
            if 1 <= step <= n_r:
                for d in (0, 1):
                    q_ring[w][d].arrive(step)
                    q_ring[w][d].start(step + 1)
                for d in (0, 1):
                    y_start(w, step, d, 1)
        step = it - PREFIX_LAG
        if step == 0:
            for d in (0, 1):
                prefix[d].start(1)
        if 1 <= step <= n_r:
            for d in (0, 1):
                prefix[d].arrive(step)
                prefix[d].start(step + 1)
            got_ref[2 * step - 1] = pg_r[starts_r[step - 1]]
            if step <= n_l:
                got_ref[2 * step] = pg_l[starts_l[step - 1]]
        step = it - fresh_from
        if 1 <= step <= n_r:
            for d in (0, 1):
                fresh[d].arrive(step)
                fresh[d].start(step + 1)
            fresh_ref[origin(0, step)] = fg_r[starts_r[step - 1]]
            if step <= n_l:
                fresh_ref[origin(1, step)] = fg_l[starts_l[step - 1]]
        for hop in range(1, y_max + 1):
            for w in (0, 1):
                step = it - w * n_r - hop
                if 1 <= step <= n_r:
                    for d in (0, 1):
                        y_arrive(w, step, d, hop)
                        y_start(w, step, d, hop + 1)
        if it == 1:
            pending += [("kv", 0), (0, 0), (1, 0)]
        if it <= n_r:
            pending.append(("kv", it))
        for w in (0, 1):
            step = it - w * n_r - y_max
            if 1 <= step <= n_r:
                pending.append((w, step))
        if it == 3:
            tokens_near()
        if it == NORM_AT - 1:
            tokens_far()
        if it == NORM_AT:
            normalise()
        if it > NORM_AT:
            if it == n_r:
                pending.sort(key=lambda item: item[0] != "kv")
            take = len([1 for item in pending if item[0] == "kv"]) if it == n_r else 0
            take = len(pending) if it == last else max(take, CATCH_UP)
            for kind, step in pending[:take]:
                if kind == "kv":
                    kv_product(step)
                else:
                    q_product(kind, step)
            pending = pending[take:]
        if it == n_r:
            finish_kv()
        if it == fresh_from:
            for d in (0, 1):
                fresh[d].start(1)

    for pair in [kv, *q_ring, prefix, fresh]:
        for one in pair:
            one.drain()
    for copy in [*y_open.values(), *tok_open, *gain_open]:
        copy.wait_send()


def attend_kernel(
    q0_ref, q1_ref, bq_ref, cos_ref, sin_ref, knew_ref, vnew_ref, got_ref, at_ref, plen_ref, slen_ref,
    out_ref, kall, vall,
):
    rows = q0_ref.shape[0]
    requests = rows // BLOCK
    slots = at_ref.shape[0] // requests
    old = slots * PAGE
    per = q0_ref.shape[1] // HEAD_DIM
    for b in range(requests):
        def page(j, carry):
            index = at_ref[b * slots + j]
            to = pl.ds(pl.multiple_of(j * PAGE, PAGE), PAGE)
            kall[b, to, :] = got_ref[index, 0].astype(jnp.float32)
            vall[b, to, :] = got_ref[index, 1].astype(jnp.float32)
            return carry

        lax.fori_loop(0, slots, page, 0)
        mine = slice(b * BLOCK, (b + 1) * BLOCK)
        kall[b, old:, :] = knew_ref[mine, :].astype(jnp.float32)
        vall[b, old:, :] = vnew_ref[mine, :].astype(jnp.float32)
        keys = kall[b].astype(jnp.bfloat16)
        values = vall[b].astype(jnp.bfloat16)
        key_pos = lax.broadcasted_iota(jnp.int32, (BLOCK, old + BLOCK), 1)
        query_pos = lax.broadcasted_iota(jnp.int32, (BLOCK, old + BLOCK), 0)
        shifted = key_pos - old
        allowed = ((shifted < 0) & (key_pos < plen_ref[b])) | (
            (shifted >= 0) & (shifted <= query_pos) & (shifted < slen_ref[b])
        )
        live = lax.broadcasted_iota(jnp.int32, (BLOCK, HEAD_DIM), 0) < slen_ref[b]
        cos, sin = cos_ref[mine, :], sin_ref[mine, :]
        for h in range(2 * per):
            lin = (q0_ref, q1_ref)[h // per][mine, (h % per) * HEAD_DIM : (h % per + 1) * HEAD_DIM]
            lin = lin + bq_ref[:, h * HEAD_DIM : (h + 1) * HEAD_DIM]
            query = (lin * cos + pltpu.roll(lin, HEAD_DIM // 2, 1) * sin).astype(jnp.bfloat16)
            scores = lax.dot_general(
                query, keys, (((1,), (1,)), ((), ())), preferred_element_type=jnp.float32
            ) * (1.0 / math.sqrt(HEAD_DIM))
            masked = jnp.where(allowed, scores, -1e30)
            peak = jnp.max(masked, axis=1, keepdims=True)
            weights = jnp.where(allowed, jnp.exp(masked - peak), 0.0)
            probs = (weights / jnp.sum(weights, axis=1, keepdims=True)).astype(jnp.bfloat16)
            mixed = jnp.dot(probs, values, preferred_element_type=jnp.float32)
            out_ref[mine, h * HEAD_DIM : (h + 1) * HEAD_DIM] = jnp.where(live, mixed, 0.0).astype(
                jnp.bfloat16
            )


def body(
    n_parts,
    tokens, norm_gain, w_query, w_kv, b_query, b_kv, kv_pool, prefix_pages, prefix_len, suffix_len,
    fresh_owner,
):
    n_seq, n_tp = lax.axis_size("seq"), lax.axis_size("tp")
    me = lax.axis_index("seq")
    rows, features = tokens.shape
    requests = rows // BLOCK
    depth, query_width = w_query.shape
    kv_width = w_kv.shape[2]
    pool_pages = kv_pool.shape[0]
    slots = prefix_pages.shape[1]
    entries = requests * slots
    suffix_pages = BLOCK // PAGE
    fresh_entries = requests * suffix_pages
    prefix_cap = max(3, entries // n_seq + 1)
    fresh_cap = max(2, (fresh_entries + n_seq - 1) // n_seq + 1)
    n_r, n_l = n_seq // 2, (n_seq - 1) // 2
    first_row = me * requests
    prefix_mine = lax.dynamic_slice_in_dim(prefix_len, first_row, requests)
    suffix_mine = lax.dynamic_slice_in_dim(suffix_len, first_row, requests)
    owners_mine = lax.dynamic_slice_in_dim(fresh_owner[:, 0], first_row * suffix_pages, fresh_entries)
    steps = jnp.asarray(
        [0] + list(range(1, n_r + 1)) + [n_seq - k for k in range(1, n_l + 1)], jnp.int32
    )
    around = lax.rem(me + steps, n_seq)

    all_ids = prefix_pages.reshape(n_seq, entries)
    all_owner = all_ids // pool_pages
    entry = jnp.arange(entries, dtype=jnp.int32)
    earlier = entry[None, :] < entry[:, None]
    mine_here = all_owner == me
    before = jnp.sum(
        (mine_here[:, None, :] & earlier[None]).astype(jnp.int32), axis=-1
    )
    cap_ids = jnp.arange(prefix_cap, dtype=jnp.int32)
    chosen = mine_here[:, None, :] & (before[:, None, :] == cap_ids[None, :, None])
    local_page = jnp.sum(jnp.where(chosen, (all_ids % pool_pages)[:, None, :], 0), axis=-1)
    prefix_send = kv_pool[local_page[around]]

    my_ids = lax.dynamic_index_in_dim(all_ids, me, 0, keepdims=False)
    my_owner = my_ids // pool_pages
    my_rank = jnp.sum(((my_owner[None, :] == my_owner[:, None]) & earlier).astype(jnp.int32), axis=1)
    distance = lax.rem(me - my_owner + n_seq, n_seq)
    place = jnp.where(
        distance == 0, 0, jnp.where(distance <= n_r, 2 * distance - 1, 2 * (n_seq - distance))
    )
    arrived_at = place * prefix_cap + my_rank

    fresh_ids = jnp.arange(fresh_entries, dtype=jnp.int32)
    fresh_rank = jnp.sum(
        (
            (owners_mine[None, :] == owners_mine[:, None])
            & (fresh_ids[None, :] < fresh_ids[:, None])
        ).astype(jnp.int32),
        axis=1,
    )
    placed = (owners_mine[None, None, :] == around[:, None, None]) & (
        fresh_rank[None, None, :] == jnp.arange(fresh_cap, dtype=jnp.int32)[None, :, None]
    )
    source = jnp.sum(jnp.where(placed, fresh_ids[None, None, :] - fresh_entries, 0), axis=-1)
    source = (source + fresh_entries).reshape(-1)

    half_dim = HEAD_DIM // 2
    slot_ids = jnp.arange(BLOCK, dtype=jnp.int32)
    positions = (prefix_mine[:, None] + slot_ids[None, :]).reshape(rows, 1)
    inverse = jnp.exp(
        jnp.arange(half_dim, dtype=jnp.float32) * (-2.0 * math.log(1000000.0) / HEAD_DIM)
    )
    angles = positions.astype(jnp.float32) * inverse
    cosine, sine = jnp.cos(angles), jnp.sin(angles)
    cos_all = jnp.concatenate([cosine, cosine], axis=1)
    sin_all = jnp.concatenate([-sine, sine], axis=1)
    live = (slot_ids[None, :] < suffix_mine[:, None]).reshape(rows, 1)
    live_all = jnp.broadcast_to(live.astype(jnp.float32), (rows, HEAD_DIM))

    q_cols = query_width // 2
    piece = depth // n_parts
    y_lanes = max(1, n_parts - 1)
    tri_r, tri_l = offsets(n_r)[1], offsets(n_l)[1]
    page = (2, PAGE, HEAD_DIM)
    bf16, f32 = jnp.bfloat16, jnp.float32
    vmem = pl.BlockSpec(memory_space=pltpu.VMEM)
    smem = pl.BlockSpec(memory_space=pltpu.SMEM)
    dma = pltpu.SemaphoreType.DMA
    q0, q1, knew, vnew, got, fresh = pl.pallas_call(
        functools.partial(gather_kernel, n_parts, n_seq, n_tp),
        name="gather",
        out_shape=(
            jax.ShapeDtypeStruct((rows, q_cols), f32),
            jax.ShapeDtypeStruct((rows, q_cols), f32),
            jax.ShapeDtypeStruct((rows, HEAD_DIM), bf16),
            jax.ShapeDtypeStruct((rows, HEAD_DIM), bf16),
            jax.ShapeDtypeStruct((n_seq, prefix_cap, *page), bf16),
            jax.ShapeDtypeStruct((n_seq, fresh_cap, *page), bf16),
        ),
        in_specs=[vmem] * 9 + [smem],
        out_specs=(vmem,) * 6,
        scratch_shapes=[
            pltpu.VMEM((n_tp, rows, features), bf16),
            pltpu.VMEM((n_tp, 1, features), f32),
            pltpu.VMEM((n_seq, rows, depth), bf16),
            pltpu.VMEM((n_seq, depth, 2 * kv_width), bf16),
            pltpu.VMEM((n_seq, n_parts, piece, q_cols), bf16),
            pltpu.VMEM((n_seq, n_parts, piece, q_cols), bf16),
            pltpu.VMEM((rows, 2 * kv_width), f32),
            pltpu.VMEM((tri_r, prefix_cap, *page), bf16),
            pltpu.VMEM((tri_l, prefix_cap, *page), bf16),
            pltpu.VMEM((n_seq, fresh_cap, *page), bf16),
            pltpu.VMEM((tri_r, fresh_cap, *page), bf16),
            pltpu.VMEM((tri_l, fresh_cap, *page), bf16),
            pltpu.VMEM((fresh_entries + 1, *page), bf16),
            dma((5, 2, 2)),
            dma((5, 2, n_r)),
            dma((2, y_lanes, 2)),
            dma((2, y_lanes, n_r)),
            dma((9,)),
            dma((9,)),
            dma((n_tp - 1,)),
            dma((n_tp - 1,)),
        ],
        compiler_params=pltpu.CompilerParams(
            collective_id=0, has_side_effects=True, vmem_limit_bytes=60 * 1024 * 1024
        ),
    )(
        tokens,
        norm_gain.astype(f32).reshape(1, features),
        w_kv.reshape(depth, 2 * kv_width),
        w_query.reshape(n_parts, piece, query_width),
        b_kv.reshape(1, 2 * kv_width),
        cos_all,
        sin_all,
        live_all,
        prefix_send,
        source,
    )
    attn_out = pl.pallas_call(
        attend_kernel,
        name="attend",
        out_shape=jax.ShapeDtypeStruct((rows, query_width), bf16),
        in_specs=[vmem] * 8 + [smem] * 3,
        out_specs=vmem,
        scratch_shapes=[
            pltpu.VMEM((requests, slots * PAGE + BLOCK, HEAD_DIM), f32),
            pltpu.VMEM((requests, slots * PAGE + BLOCK, HEAD_DIM), f32),
        ],
    )(
        q0,
        q1,
        b_query.reshape(1, query_width),
        cos_all,
        sin_all,
        knew,
        vnew,
        got.reshape(n_seq * prefix_cap, *page),
        arrived_at,
        prefix_mine,
        suffix_mine,
    )
    return attn_out, fresh.reshape(n_seq * fresh_cap, *page)


def solution(mesh):
    placed = (
        P(("parts", "seq"), "tp"),
        P("tp"),
        P("seq", "tp"),
        P("seq", None, "tp"),
        P("tp"),
        P(None, "tp"),
        P(("parts", "seq"), None, None, "tp"),
        P("parts", None),
        P("parts"),
        P("parts"),
        P("parts", None),
    )
    return jax.shard_map(
        functools.partial(body, mesh.shape["parts"]),
        mesh=mesh,
        in_specs=placed,
        out_specs=(P(("parts", "seq"), "tp"), P(("parts", "seq"), None, None, "tp")),
        check_vma=False,
    )
```

```python
import functools
import math

import jax
import jax.numpy as jnp
from jax import lax
from jax.experimental import pallas as pl
from jax.experimental.pallas import tpu as pltpu
from jax.sharding import PartitionSpec as P

HEAD_DIM = 128
BLOCK = 128
PAGE = 8
MESH = pl.DeviceIdType.MESH

PREFIX_LAG = 6
Z_LAG = (0, 1, 3)
Y_WAIT = (0, 0, 8)
GROUPS_AT_ONCE = 2


def offsets(count):
    starts, at = [], 0
    for step in range(1, count + 1):
        starts.append(at)
        at += count - step + 1
    return starts, at


class Ring:
    def __init__(self, make, steps):
        self.make, self.steps, self.started = make, steps, {}

    def start(self, step):
        if step > self.steps:
            return
        if step > 2:
            self.started.pop(step - 2).wait_send()
        copy = self.make(step)
        copy.start()
        self.started[step] = copy

    def arrive(self, step):
        if step <= self.steps:
            self.make(step).wait_recv()

    def drain(self):
        for copy in self.started.values():
            copy.wait_send()
        self.started = {}


def gather_kernel(
    n_parts, n_seq, n_tp,
    tok_ref, gain_ref, wkv_ref, wq_ref, bkv_ref, cos_ref, sin_ref, pool_ref,
    pages_ref, plen_ref, slen_ref, owner_ref,
    q0_ref, q1_ref, knew_ref, vnew_ref, got_ref, fresh_ref,
    toks, gains, nrm, wkvb, wqb0, wqb1, acc, psend, pg_r, pg_l, fsend, fgot, newp, source,
    ring_send, ring_recv, y_send, y_recv, tok_send, tok_recv, gain_send, gain_recv,
    fresh_send, fresh_recv,
):
    part, me, tp = lax.axis_index("parts"), lax.axis_index("seq"), lax.axis_index("tp")
    right, left = lax.rem(me + 1, n_seq), lax.rem(me + n_seq - 1, n_seq)
    up, down = lax.rem(part + 1, n_parts), lax.rem(part + n_parts - 1, n_parts)
    n_r, n_l = n_seq // 2, (n_seq - 1) // 2
    y_r, y_l = n_parts // 2, (n_parts - 1) // 2
    y_max = max(y_r, y_l)
    partner = tp + 1 - 2 * lax.rem(tp, 2)
    x_right, x_left = lax.rem(tp + 2, n_tp), lax.rem(tp + n_tp - 2, n_tp)
    x_far = lax.rem(tp + n_tp // 2, n_tp)
    rows, features = tok_ref.shape
    half = rows // 2
    depth = wkv_ref.shape[0] * wkv_ref.shape[1]
    q_cols = q0_ref.shape[1]
    pool_pages = pool_ref.shape[0]
    requests = rows // BLOCK
    fresh_entries = rows // PAGE
    prefix_cap, fresh_cap = psend.shape[1], fsend.shape[1]

    barrier = pltpu.get_barrier_semaphore()
    greeted = [{"seq": right}, {"seq": left}]
    greeted += [{"tp": lax.rem(tp + r, n_tp)} for r in range(1, n_tp)]
    if n_parts > 1:
        greeted.append({"parts": up})
    if n_parts > 2:
        greeted.append({"parts": down})
    for device in greeted:
        pl.semaphore_signal(barrier, inc=1, device_id=device, device_id_type=MESH)
    pl.semaphore_wait(barrier, len(greeted))

    def remote(src, dst, send, recv, device):
        return pltpu.make_async_remote_copy(
            src_ref=src, dst_ref=dst, send_sem=send, recv_sem=recv,
            device_id=device, device_id_type=MESH,
        )

    def origin(direction, step):
        return lax.rem(me + (n_seq - step if direction == 0 else step), n_seq)

    def around(index):
        by = jnp.where(index <= n_r, index, n_seq + n_r - index)
        return lax.rem(me + by, n_seq)

    def slot(direction, step):
        return 2 * step - 1 if direction == 0 else 2 * step

    def ring(stream, direction, make_refs):
        target = {"seq": right if direction == 0 else left}

        def make(step):
            src, dst = make_refs(step)
            return remote(
                src, dst, ring_send.at[stream, direction, step % 2],
                ring_recv.at[stream, direction, step - 1], target,
            )

        return Ring(make, n_r if direction == 0 else n_l)

    buffers = (wkvb, wqb0, wqb1)
    owns = (
        lambda: wkv_ref.at[part],
        lambda: wq_ref.at[part, :, pl.ds(0, q_cols)],
        lambda: wq_ref.at[part, :, pl.ds(q_cols, q_cols)],
    )

    def weight_refs(which, direction):
        def refs(step):
            if step == 1:
                src = owns[which]()
            else:
                src = buffers[which].at[slot(direction, step - 1), part]
            return src, buffers[which].at[slot(direction, step), part]

        return refs

    starts = (offsets(n_r)[0], offsets(n_l)[0])

    def prefix_refs(direction):
        count, buffer = ((n_r, pg_r), (n_l, pg_l))[direction]

        def refs(step):
            size = count - step + 1
            if step == 1:
                src = psend.at[pl.ds(1 if direction == 0 else 1 + n_r, count)]
            else:
                src = buffer.at[pl.ds(starts[direction][step - 2] + 1, size)]
            return src, buffer.at[pl.ds(starts[direction][step - 1], size)]

        return refs

    weights = [[ring(w, d, weight_refs(w, d)) for d in (0, 1)] for w in range(3)]
    prefix = [ring(3, d, prefix_refs(d)) for d in (0, 1)]

    y_open = {}

    def y_make(which, step, direction, hop, behind):
        by = hop - 1 + behind
        piece = lax.rem(part + (n_parts - by if direction == 0 else by), n_parts)
        pair = pl.ds(2 * step - 1, 2 if step <= n_l else 1)
        ref = buffers[which].at[pair, piece]
        lane = hop - 1 if direction == 0 else y_r + hop - 1
        return remote(
            ref, ref, y_send.at[which, lane, step % 2], y_recv.at[which, lane, step - 1],
            {"parts": up if direction == 0 else down},
        )

    def y_start(which, step, direction, hop):
        if hop > (y_r if direction == 0 else y_l):
            return
        key = (which, direction, hop)
        if (key, step - 2) in y_open:
            y_open.pop((key, step - 2)).wait_send()
        copy = y_make(which, step, direction, hop, 0)
        copy.start()
        y_open[(key, step)] = copy

    def y_arrive(which, step, direction, hop):
        if hop <= (y_r if direction == 0 else y_l):
            y_make(which, step, direction, hop, 1).wait_recv()

    lo, hi = pl.ds(0, half), pl.ds(half, half)

    def tok_copy(index, src, block, part_rows, device):
        dst = toks.at[block] if part_rows is None else toks.at[block, part_rows]
        if src is None:
            src = dst
        return remote(src, dst, tok_send.at[index], tok_recv.at[index], {"tp": device})

    opened = []

    def tok_start(*args):
        copy = tok_copy(*args)
        copy.start()
        opened.append(copy)

    for d in (0, 1):
        weights[0][d].start(1)
    tok_start(1, tok_ref, tp, None, x_right)
    tok_start(2, tok_ref, tp, None, x_left)
    tok_start(0, tok_ref, tp, None, partner)
    for r in range(1, n_tp):
        copy = remote(
            gain_ref, gains.at[tp], gain_send.at[r - 1], gain_recv.at[r - 1],
            {"tp": lax.rem(tp + r, n_tp)},
        )
        copy.start()
        opened.append(copy)
    toks[tp] = tok_ref[...]
    gains[tp] = gain_ref[...]
    acc[...] = jnp.zeros_like(acc)
    q0_ref[...] = jnp.zeros_like(q0_ref)
    q1_ref[...] = jnp.zeros_like(q1_ref)

    def tokens_near():
        tok_copy(1, None, x_left, None, x_right).wait_recv()
        tok_start(5, None, x_left, lo, x_right)
        tok_start(3, None, x_left, None, partner)
        tok_copy(2, None, x_right, None, x_left).wait_recv()
        tok_start(6, None, x_right, hi, x_left)
        tok_start(4, None, x_right, None, partner)

    def tokens_far():
        tok_copy(5, None, x_far, lo, x_right).wait_recv()
        tok_start(7, None, x_far, lo, partner)
        tok_copy(6, None, x_far, hi, x_left).wait_recv()
        tok_start(8, None, x_far, hi, partner)

    def shifted(base, by):
        return lax.rem(base + by, n_tp)

    def tokens_here():
        p_left, p_right = shifted(partner, n_tp - 2), shifted(partner, 2)
        p_far = shifted(partner, n_tp // 2)
        for index, block, part_rows in (
            (0, partner, None), (3, p_left, None), (4, p_right, None),
            (7, p_far, lo), (8, p_far, hi),
        ):
            tok_copy(index, None, block, part_rows, partner).wait_recv()
        for r in range(1, n_tp):
            remote(
                gain_ref, gains.at[lax.rem(tp + n_tp - r, n_tp)],
                gain_send.at[r - 1], gain_recv.at[r - 1], {"tp": lax.rem(tp + r, n_tp)},
            ).wait_recv()

    def normalise(first, count):
        step_rows = 16

        def some_rows(i, carry):
            at = pl.ds(pl.multiple_of(i * step_rows, step_rows), step_rows)
            total = jnp.zeros((step_rows, features), jnp.float32)
            for t in range(n_tp):
                wide = toks[t, at, :].astype(jnp.float32)
                total = total + wide * wide
            mean = jnp.sum(total, axis=1, keepdims=True) / (n_tp * features)
            scale = lax.rsqrt(mean + 1e-06)
            for t in range(n_tp):
                wide = toks[t, at, :].astype(jnp.float32)
                value = (wide * scale * gains[t]).astype(jnp.bfloat16)
                for j in range(features // depth):
                    nrm[t * (features // depth) + j, at, :] = value[:, j * depth : (j + 1) * depth]
            return carry

        lax.fori_loop(first // step_rows, (first + count) // step_rows, some_rows, 0)

    def dot(shard, weight):
        return jnp.dot(
            nrm[shard], weight.reshape(depth, -1), preferred_element_type=jnp.float32
        )

    sums = (acc, q0_ref, q1_ref)
    done = [0, 0, 0]

    def product(which, step):
        done[which] += 1
        if step == 0:
            own = wkv_ref[...] if which == 0 else wq_ref[:, :, (which - 1) * q_cols : which * q_cols]
            sums[which][...] += dot(me, own)
            return
        total = dot(origin(0, step), buffers[which][2 * step - 1])
        if step <= n_l:
            total = total + dot(origin(1, step), buffers[which][2 * step])
        sums[which][...] += total

    def pick_pages(first):
        def one(index, carry):
            group = around(index)

            def entry(j, state):
                count, picks = state
                for r in range(requests):
                    local = pages_ref[j, group * requests + r] - me * pool_pages
                    hit = jnp.where((local >= 0) & (local < pool_pages), 1, 0)
                    picks = tuple(
                        jnp.where((hit == 1) & (count == c), local, p) for c, p in enumerate(picks)
                    )
                    count = count + hit
                return count, picks

            zero = jnp.int32(0)
            _, picks = lax.fori_loop(
                0, pages_ref.shape[0], entry, (zero, (zero,) * prefix_cap), unroll=4
            )
            for c in range(prefix_cap):
                psend[index, c] = pool_ref[picks[c]]
            return carry

        lax.fori_loop(first, first + GROUPS_AT_ONCE, one, 0)

    def pick_source(first):
        def one(index, carry):
            group = around(index)

            def entry(e, state):
                count, picks = state
                hit = jnp.where(owner_ref[me * fresh_entries + e] == group, 1, 0)
                picks = tuple(
                    jnp.where((hit == 1) & (count == c), e, p) for c, p in enumerate(picks)
                )
                return count + hit, picks

            none = jnp.int32(fresh_entries)
            _, picks = lax.fori_loop(
                0, fresh_entries, entry, (jnp.int32(0), (none,) * fresh_cap), unroll=4
            )
            for c in range(fresh_cap):
                source[index * fresh_cap + c] = picks[c]
            return carry

        lax.fori_loop(first, first + GROUPS_AT_ONCE, one, 0)

    def finish_kv():
        for b in range(requests):
            mine = slice(b * BLOCK, (b + 1) * BLOCK)
            pair = acc[mine, :] + bkv_ref[...]
            key, value = pair[:, :HEAD_DIM], pair[:, HEAD_DIM:]
            at = pl.ds(plen_ref[me * requests + b], BLOCK)
            turned = key * cos_ref[at, :] + pltpu.roll(key, HEAD_DIM // 2, 1) * sin_ref[at, :]
            index = lax.broadcasted_iota(jnp.int32, (BLOCK, HEAD_DIM), 0)
            live = index < slen_ref[me * requests + b]
            key = jnp.where(live, turned, 0.0)
            value = jnp.where(live, value, 0.0)
            knew_ref[mine, :] = key.astype(jnp.bfloat16)
            vnew_ref[mine, :] = value.astype(jnp.bfloat16)
            count = BLOCK // PAGE
            pages = pl.ds(b * count, count)
            newp[pages, 0] = key.reshape(count, PAGE, HEAD_DIM).astype(jnp.bfloat16)
            newp[pages, 1] = value.reshape(count, PAGE, HEAD_DIM).astype(jnp.bfloat16)
        newp[fresh_entries] = jnp.zeros((2, PAGE, HEAD_DIM), jnp.bfloat16)

        def select(i, carry):
            for c in range(fresh_cap):
                fsend[i, c] = newp[source[i * fresh_cap + c]]
            return carry

        lax.fori_loop(0, n_seq, select, 0)
        fgot[me] = fsend[0]

    def fresh_copy(direction, step, behind):
        index = step if direction == 0 else n_r + step
        group = origin(1 - direction, step)
        there = me if not behind else origin(direction, step)
        return remote(
            fsend.at[index], fgot.at[there], fresh_send.at[index - 1], fresh_recv.at[index - 1],
            {"seq": group},
        )

    far_first = [
        (d, step) for step in range(n_r, 0, -1) for d in (0, 1) if step <= (n_r if d == 0 else n_l)
    ]

    work = []

    def fill(count):
        for _ in range(min(count, len(work))):
            work.pop(0)()

    work += [functools.partial(pick_pages, i) for i in range(0, n_seq, GROUPS_AT_ONCE)]
    sources = [functools.partial(pick_source, i) for i in range(0, n_seq, GROUPS_AT_ONCE)]
    products = []

    def compute(count):
        for _ in range(min(count, len(products))):
            product(*products.pop(0))

    wait = y_max + 1 if y_max else 0
    kv_end = n_r + Z_LAG[0] + Y_WAIT[0] + wait
    last = max(max(n_r + z + y + wait for z, y in zip(Z_LAG, Y_WAIT)), n_r + PREFIX_LAG)
    ready = 7
    for it in range(1, last + 1):
        busy = compute if it > ready else fill
        for w in range(3):
            step = it - Z_LAG[w]
            if step == 0:
                for d in (0, 1):
                    weights[w][d].start(1)
            if 1 <= step <= n_r:
                for d in (0, 1):
                    weights[w][d].arrive(step)
                    weights[w][d].start(step + 1)
            step -= Y_WAIT[w]
            if 1 <= step <= n_r:
                for d in (0, 1):
                    y_start(w, step, d, 1)
            busy(1)
        step = it - PREFIX_LAG
        if step == 0:
            fill(len(work))
            got_ref[0] = psend[0]
            for d in (0, 1):
                prefix[d].start(1)
            work += sources
        if 1 <= step <= n_r:
            for d in (0, 1):
                prefix[d].arrive(step)
                prefix[d].start(step + 1)
            got_ref[2 * step - 1] = pg_r[starts[0][step - 1]]
            if step <= n_l:
                got_ref[2 * step] = pg_l[starts[1][step - 1]]
        busy(1)
        for w in range(3):
            for hop in range(1, y_max + 1):
                step = it - Z_LAG[w] - Y_WAIT[w] - hop - 1
                if 1 <= step <= n_r:
                    for d in (0, 1):
                        y_arrive(w, step, d, hop)
                        y_start(w, step, d, hop + 1)
            step = it - Z_LAG[w] - Y_WAIT[w] - wait
            if 0 <= step <= n_r:
                products.append((w, step))
        if it == 3:
            tokens_near()
        if it == ready - 2:
            tokens_far()
        if it == ready - 1:
            tokens_here()
            normalise(0, half)
        if it == ready:
            normalise(half, half)
        if it > ready:
            fill(1)
        if it == kv_end:
            fill(len(work))
            products.sort(key=lambda item: item[0])
            compute(len([item for item in products if item[0] == 0]))
            finish_kv()
            for d, step in far_first:
                copy = fresh_copy(d, step, False)
                copy.start()
                opened.append(copy)
    compute(len(products))
    assert done == [n_r + 1] * 3 and not work

    for d, step in far_first:
        fresh_copy(d, step, True).wait_recv()
    fresh_ref[...] = fgot[...]
    for pair in [*weights, prefix]:
        for one in pair:
            one.drain()
    for copy in [*y_open.values(), *opened]:
        copy.wait_send()


def attend_kernel(
    n_seq, pool_pages,
    q0_ref, q1_ref, bq_ref, cos_ref, sin_ref, knew_ref, vnew_ref, got_ref,
    pages_ref, plen_ref, slen_ref,
    out_ref, kall, vall, counts,
):
    me = lax.axis_index("seq")
    rows = q0_ref.shape[0]
    requests = rows // BLOCK
    slots = pages_ref.shape[0]
    old = slots * PAGE
    per = q0_ref.shape[1] // HEAD_DIM
    cap = got_ref.shape[0] // n_seq
    n_r = n_seq // 2

    def clear(i, carry):
        counts[i] = 0
        return carry

    lax.fori_loop(0, n_seq, clear, 0)

    def page(j, carry):
        to = pl.ds(pl.multiple_of(j * PAGE, PAGE), PAGE)
        for b in range(requests):
            owner = lax.div(pages_ref[j, me * requests + b], pool_pages)
            rank = counts[owner]
            counts[owner] = rank + 1
            away = me - owner
            away = jnp.where(away < 0, away + n_seq, away)
            place = jnp.where(away <= n_r, 2 * away - 1, 2 * (n_seq - away))
            place = jnp.where(away == 0, 0, place)
            index = place * cap + rank
            kall[b, to, :] = got_ref[index, 0].astype(jnp.float32)
            vall[b, to, :] = got_ref[index, 1].astype(jnp.float32)
        return carry

    lax.fori_loop(0, slots, page, 0, unroll=4)
    for b in range(requests):
        mine = slice(b * BLOCK, (b + 1) * BLOCK)
        kall[b, old:, :] = knew_ref[mine, :].astype(jnp.float32)
        vall[b, old:, :] = vnew_ref[mine, :].astype(jnp.float32)
        keys = kall[b].astype(jnp.bfloat16)
        values = vall[b].astype(jnp.bfloat16)
        here = me * requests + b
        key_pos = lax.broadcasted_iota(jnp.int32, (BLOCK, old + BLOCK), 1)
        query_pos = lax.broadcasted_iota(jnp.int32, (BLOCK, old + BLOCK), 0)
        shifted = key_pos - old
        allowed = ((shifted < 0) & (key_pos < plen_ref[here])) | (
            (shifted >= 0) & (shifted <= query_pos) & (shifted < slen_ref[here])
        )
        live = lax.broadcasted_iota(jnp.int32, (BLOCK, HEAD_DIM), 0) < slen_ref[here]
        at = pl.ds(plen_ref[here], BLOCK)
        cos, sin = cos_ref[at, :], sin_ref[at, :]
        for h in range(2 * per):
            lin = (q0_ref, q1_ref)[h // per][mine, (h % per) * HEAD_DIM : (h % per + 1) * HEAD_DIM]
            lin = lin + bq_ref[:, h * HEAD_DIM : (h + 1) * HEAD_DIM]
            query = (lin * cos + pltpu.roll(lin, HEAD_DIM // 2, 1) * sin).astype(jnp.bfloat16)
            scores = lax.dot_general(
                query, keys, (((1,), (1,)), ((), ())), preferred_element_type=jnp.float32
            ) * (1.0 / math.sqrt(HEAD_DIM))
            masked = jnp.where(allowed, scores, -1e30)
            peak = jnp.max(masked, axis=1, keepdims=True)
            weights = jnp.where(allowed, jnp.exp(masked - peak), 0.0)
            probs = (weights * (1.0 / jnp.sum(weights, axis=1, keepdims=True))).astype(jnp.bfloat16)
            mixed = jnp.dot(probs, values, preferred_element_type=jnp.float32)
            out_ref[mine, h * HEAD_DIM : (h + 1) * HEAD_DIM] = jnp.where(live, mixed, 0.0).astype(
                jnp.bfloat16
            )


def body(
    n_parts,
    tokens, norm_gain, w_query, w_kv, b_query, b_kv, kv_pool, prefix_pages, prefix_len, suffix_len,
    fresh_owner,
):
    n_seq, n_tp = lax.axis_size("seq"), lax.axis_size("tp")
    rows, features = tokens.shape
    requests = rows // BLOCK
    depth, query_width = w_query.shape
    kv_width = w_kv.shape[2]
    pool_pages = kv_pool.shape[0]
    slots = prefix_pages.shape[1]
    entries = requests * slots
    fresh_entries = rows // PAGE
    prefix_cap = max(3, entries // n_seq + 1)
    fresh_cap = max(2, (fresh_entries + n_seq - 1) // n_seq + 1)
    n_r, n_l = n_seq // 2, (n_seq - 1) // 2

    half_dim = HEAD_DIM // 2
    positions = jnp.arange(slots * PAGE + BLOCK, dtype=jnp.float32)[:, None]
    inverse = jnp.exp(
        jnp.arange(half_dim, dtype=jnp.float32) * (-2.0 * math.log(1000000.0) / HEAD_DIM)
    )
    angles = positions * inverse
    cosine, sine = jnp.cos(angles), jnp.sin(angles)
    cos_all = jnp.concatenate([cosine, cosine], axis=1)
    sin_all = jnp.concatenate([-sine, sine], axis=1)
    pages_by_slot = prefix_pages.T

    q_cols = query_width // 2
    piece = depth // n_parts
    y_lanes = max(1, n_parts - 1)
    tri_r, tri_l = offsets(n_r)[1], offsets(n_l)[1]
    page = (2, PAGE, HEAD_DIM)
    bf16, f32 = jnp.bfloat16, jnp.float32
    vmem = pl.BlockSpec(memory_space=pltpu.VMEM)
    smem = pl.BlockSpec(memory_space=pltpu.SMEM)
    dma = pltpu.SemaphoreType.DMA
    q0, q1, knew, vnew, got, fresh = pl.pallas_call(
        functools.partial(gather_kernel, n_parts, n_seq, n_tp),
        name="gather",
        out_shape=(
            jax.ShapeDtypeStruct((rows, q_cols), f32),
            jax.ShapeDtypeStruct((rows, q_cols), f32),
            jax.ShapeDtypeStruct((rows, HEAD_DIM), bf16),
            jax.ShapeDtypeStruct((rows, HEAD_DIM), bf16),
            jax.ShapeDtypeStruct((n_seq, prefix_cap, *page), bf16),
            jax.ShapeDtypeStruct((n_seq, fresh_cap, *page), bf16),
        ),
        in_specs=[vmem] * 8 + [smem] * 4,
        out_specs=(vmem,) * 6,
        scratch_shapes=[
            pltpu.VMEM((n_tp, rows, features), bf16),
            pltpu.VMEM((n_tp, 1, features), f32),
            pltpu.VMEM((n_seq, rows, depth), bf16),
            pltpu.VMEM((n_seq, n_parts, piece, 2 * kv_width), bf16),
            pltpu.VMEM((n_seq, n_parts, piece, q_cols), bf16),
            pltpu.VMEM((n_seq, n_parts, piece, q_cols), bf16),
            pltpu.VMEM((rows, 2 * kv_width), f32),
            pltpu.VMEM((n_seq, prefix_cap, *page), bf16),
            pltpu.VMEM((tri_r, prefix_cap, *page), bf16),
            pltpu.VMEM((tri_l, prefix_cap, *page), bf16),
            pltpu.VMEM((n_seq, fresh_cap, *page), bf16),
            pltpu.VMEM((n_seq, fresh_cap, *page), bf16),
            pltpu.VMEM((fresh_entries + 1, *page), bf16),
            pltpu.SMEM((n_seq * fresh_cap,), jnp.int32),
            dma((4, 2, 2)),
            dma((4, 2, n_r)),
            dma((3, y_lanes, 2)),
            dma((3, y_lanes, n_r)),
            dma((9,)),
            dma((9,)),
            dma((n_tp - 1,)),
            dma((n_tp - 1,)),
            dma((n_seq - 1,)),
            dma((n_seq - 1,)),
        ],
        compiler_params=pltpu.CompilerParams(
            collective_id=0, has_side_effects=True, vmem_limit_bytes=60 * 1024 * 1024
        ),
    )(
        tokens,
        norm_gain.astype(f32).reshape(1, features),
        w_kv.reshape(n_parts, piece, 2 * kv_width),
        w_query.reshape(n_parts, piece, query_width),
        b_kv.reshape(1, 2 * kv_width),
        cos_all,
        sin_all,
        kv_pool,
        pages_by_slot,
        prefix_len,
        suffix_len,
        fresh_owner.reshape(-1),
    )
    attn_out = pl.pallas_call(
        functools.partial(attend_kernel, n_seq, pool_pages),
        name="attend",
        out_shape=jax.ShapeDtypeStruct((rows, query_width), bf16),
        in_specs=[vmem] * 8 + [smem] * 3,
        out_specs=vmem,
        scratch_shapes=[
            pltpu.VMEM((requests, slots * PAGE + BLOCK, HEAD_DIM), f32),
            pltpu.VMEM((requests, slots * PAGE + BLOCK, HEAD_DIM), f32),
            pltpu.SMEM((n_seq,), jnp.int32),
        ],
    )(
        q0,
        q1,
        b_query.reshape(1, query_width),
        cos_all,
        sin_all,
        knew,
        vnew,
        got.reshape(n_seq * prefix_cap, *page),
        pages_by_slot,
        prefix_len,
        suffix_len,
    )
    return attn_out, fresh.reshape(n_seq * fresh_cap, *page)


def solution(mesh):
    placed = (
        P(("parts", "seq"), "tp"),
        P("tp"),
        P("seq", "tp"),
        P("seq", None, "tp"),
        P("tp"),
        P(None, "tp"),
        P(("parts", "seq"), None, None, "tp"),
        P("parts", None),
        P("parts"),
        P("parts"),
        P("parts", None),
    )
    return jax.shard_map(
        functools.partial(body, mesh.shape["parts"]),
        mesh=mesh,
        in_specs=placed,
        out_specs=(P(("parts", "seq"), "tp"), P(("parts", "seq"), None, None, "tp")),
        check_vma=False,
    )
```

```python
import functools
import math

import jax
import jax.numpy as jnp
import numpy as np
from jax import lax
from jax.experimental import pallas as pl
from jax.experimental.pallas import tpu as pltpu
from jax.sharding import PartitionSpec as P

HEAD_DIM = 128
BLOCK = 128
PAGE = 8
MESH = pl.DeviceIdType.MESH

PREFIX_LAG = 4
Z_LAG = (0, 2)
Y_WAIT = (0, 3)
GROUPS_AT_ONCE = 2


def offsets(count):
    starts, at = [], 0
    for step in range(1, count + 1):
        starts.append(at)
        at += count - step + 1
    return starts, at


class Ring:
    def __init__(self, make, steps):
        self.make, self.steps, self.started = make, steps, {}

    def start(self, step):
        if step > self.steps:
            return
        if step > 2:
            self.started.pop(step - 2).wait_send()
        copy = self.make(step)
        copy.start()
        self.started[step] = copy

    def arrive(self, step):
        if step <= self.steps:
            self.make(step).wait_recv()

    def drain(self):
        for copy in self.started.values():
            copy.wait_send()
        self.started = {}


def gather_kernel(
    n_parts, n_seq, n_tp,
    tok_ref, gain_ref, wkv_ref, wq_ref, bkv_ref, cos_ref, sin_ref, pool_ref,
    pages_ref, plen_ref, slen_ref, owner_ref,
    q_ref, knew_ref, vnew_ref, got_ref, fresh_ref,
    toks, gains, nrm, wkvb, wqb, acc, psend, pg_r, pg_l, fsend, fgot, newp, source,
    ring_send, ring_recv, y_send, y_recv, tok_send, tok_recv, gain_send, gain_recv,
    fresh_send, fresh_recv,
):
    part, me, tp = lax.axis_index("parts"), lax.axis_index("seq"), lax.axis_index("tp")
    right, left = lax.rem(me + 1, n_seq), lax.rem(me + n_seq - 1, n_seq)
    up, down = lax.rem(part + 1, n_parts), lax.rem(part + n_parts - 1, n_parts)
    n_r, n_l = n_seq // 2, (n_seq - 1) // 2
    y_r, y_l = n_parts // 2, (n_parts - 1) // 2
    y_max = max(y_r, y_l)
    partner = tp + 1 - 2 * lax.rem(tp, 2)
    x_right, x_left = lax.rem(tp + 2, n_tp), lax.rem(tp + n_tp - 2, n_tp)
    x_far = lax.rem(tp + n_tp // 2, n_tp)
    rows, features = tok_ref.shape
    half = rows // 2
    depth = wkv_ref.shape[0] * wkv_ref.shape[1]
    pool_pages = pool_ref.shape[0]
    requests = rows // BLOCK
    fresh_entries = rows // PAGE
    prefix_cap, fresh_cap = psend.shape[1], fsend.shape[1]

    barrier = pltpu.get_barrier_semaphore()
    greeted = [{"seq": right}, {"seq": left}]
    greeted += [{"tp": lax.rem(tp + r, n_tp)} for r in range(1, n_tp)]
    if n_parts > 1:
        greeted.append({"parts": up})
    if n_parts > 2:
        greeted.append({"parts": down})
    for device in greeted:
        pl.semaphore_signal(barrier, inc=1, device_id=device, device_id_type=MESH)
    pl.semaphore_wait(barrier, len(greeted))

    def remote(src, dst, send, recv, device):
        return pltpu.make_async_remote_copy(
            src_ref=src, dst_ref=dst, send_sem=send, recv_sem=recv,
            device_id=device, device_id_type=MESH,
        )

    def origin(direction, step):
        return lax.rem(me + (n_seq - step if direction == 0 else step), n_seq)

    def around(index):
        by = jnp.where(index <= n_r, index, n_seq + n_r - index)
        return lax.rem(me + by, n_seq)

    def slot(direction, step):
        return 2 * step - 1 if direction == 0 else 2 * step

    def ring(stream, direction, make_refs):
        target = {"seq": right if direction == 0 else left}

        def make(step):
            src, dst = make_refs(step)
            return remote(
                src, dst, ring_send.at[stream, direction, step % 2],
                ring_recv.at[stream, direction, step - 1], target,
            )

        return Ring(make, n_r if direction == 0 else n_l)

    buffers = (wkvb, wqb)
    owns = (
        lambda: wkv_ref.at[part],
        lambda: wq_ref.at[part],
    )

    def weight_refs(which, direction):
        def refs(step):
            if step == 1:
                src = owns[which]()
            else:
                src = buffers[which].at[slot(direction, step - 1), part]
            return src, buffers[which].at[slot(direction, step), part]

        return refs

    starts = (offsets(n_r)[0], offsets(n_l)[0])

    def prefix_refs(direction):
        count, buffer = ((n_r, pg_r), (n_l, pg_l))[direction]

        def refs(step):
            size = count - step + 1
            if step == 1:
                src = psend.at[pl.ds(1 if direction == 0 else 1 + n_r, count)]
            else:
                src = buffer.at[pl.ds(starts[direction][step - 2] + 1, size)]
            return src, buffer.at[pl.ds(starts[direction][step - 1], size)]

        return refs

    weights = [[ring(w, d, weight_refs(w, d)) for d in (0, 1)] for w in range(2)]
    prefix = [ring(2, d, prefix_refs(d)) for d in (0, 1)]

    y_open = {}

    def y_make(which, step, direction, hop, behind):
        by = hop - 1 + behind
        piece = lax.rem(part + (n_parts - by if direction == 0 else by), n_parts)
        pair = pl.ds(2 * step - 1, 2 if step <= n_l else 1)
        ref = buffers[which].at[pair, piece]
        lane = hop - 1 if direction == 0 else y_r + hop - 1
        return remote(
            ref, ref, y_send.at[which, lane, step % 2], y_recv.at[which, lane, step - 1],
            {"parts": up if direction == 0 else down},
        )

    def y_start(which, step, direction, hop):
        if hop > (y_r if direction == 0 else y_l):
            return
        key = (which, direction, hop)
        if (key, step - 2) in y_open:
            y_open.pop((key, step - 2)).wait_send()
        copy = y_make(which, step, direction, hop, 0)
        copy.start()
        y_open[(key, step)] = copy

    def y_arrive(which, step, direction, hop):
        if hop <= (y_r if direction == 0 else y_l):
            y_make(which, step, direction, hop, 1).wait_recv()

    lo, hi = pl.ds(0, half), pl.ds(half, half)

    def tok_copy(index, src, block, part_rows, device):
        dst = toks.at[block] if part_rows is None else toks.at[block, part_rows]
        if src is None:
            src = dst
        return remote(src, dst, tok_send.at[index], tok_recv.at[index], {"tp": device})

    opened = []

    def tok_start(*args):
        copy = tok_copy(*args)
        copy.start()
        opened.append(copy)

    for d in (0, 1):
        weights[0][d].start(1)
    tok_start(1, tok_ref, tp, None, x_right)
    tok_start(2, tok_ref, tp, None, x_left)
    tok_start(0, tok_ref, tp, None, partner)
    for r in range(1, n_tp):
        copy = remote(
            gain_ref, gains.at[tp], gain_send.at[r - 1], gain_recv.at[r - 1],
            {"tp": lax.rem(tp + r, n_tp)},
        )
        copy.start()
        opened.append(copy)
    toks[tp] = tok_ref[...]
    gains[tp] = gain_ref[...]
    acc[...] = jnp.zeros_like(acc)
    q_ref[...] = jnp.zeros_like(q_ref)

    def tokens_near():
        tok_copy(1, None, x_left, None, x_right).wait_recv()
        tok_start(5, None, x_left, lo, x_right)
        tok_start(3, None, x_left, None, partner)
        tok_copy(2, None, x_right, None, x_left).wait_recv()
        tok_start(6, None, x_right, hi, x_left)
        tok_start(4, None, x_right, None, partner)

    def tokens_far():
        tok_copy(5, None, x_far, lo, x_right).wait_recv()
        tok_start(7, None, x_far, lo, partner)
        tok_copy(6, None, x_far, hi, x_left).wait_recv()
        tok_start(8, None, x_far, hi, partner)

    def shifted(base, by):
        return lax.rem(base + by, n_tp)

    def tokens_here():
        p_left, p_right = shifted(partner, n_tp - 2), shifted(partner, 2)
        p_far = shifted(partner, n_tp // 2)
        for index, block, part_rows in (
            (0, partner, None), (3, p_left, None), (4, p_right, None),
            (7, p_far, lo), (8, p_far, hi),
        ):
            tok_copy(index, None, block, part_rows, partner).wait_recv()
        for r in range(1, n_tp):
            remote(
                gain_ref, gains.at[lax.rem(tp + n_tp - r, n_tp)],
                gain_send.at[r - 1], gain_recv.at[r - 1], {"tp": lax.rem(tp + r, n_tp)},
            ).wait_recv()

    def normalise(first, count):
        step_rows = 16

        def some_rows(i, carry):
            at = pl.ds(pl.multiple_of(i * step_rows, step_rows), step_rows)
            total = jnp.zeros((step_rows, features), jnp.float32)
            for t in range(n_tp):
                wide = toks[t, at, :].astype(jnp.float32)
                total = total + wide * wide
            mean = jnp.sum(total, axis=1, keepdims=True) / (n_tp * features)
            scale = lax.rsqrt(mean + 1e-06)
            for t in range(n_tp):
                wide = toks[t, at, :].astype(jnp.float32)
                value = (wide * scale * gains[t]).astype(jnp.bfloat16)
                for j in range(features // depth):
                    nrm[t * (features // depth) + j, at, :] = value[:, j * depth : (j + 1) * depth]
            return carry

        lax.fori_loop(first // step_rows, (first + count) // step_rows, some_rows, 0)

    def dot(shard, weight):
        return jnp.dot(
            nrm[shard], weight.reshape(depth, -1), preferred_element_type=jnp.float32
        )

    sums = (acc, q_ref)
    done = [0, 0]

    def product(which, step):
        done[which] += 1
        if step == 0:
            own = (wkv_ref, wq_ref)[which][...]
            sums[which][...] += dot(me, own)
            return
        total = dot(origin(0, step), buffers[which][2 * step - 1])
        if step <= n_l:
            total = total + dot(origin(1, step), buffers[which][2 * step])
        sums[which][...] += total

    def pick_pages(first):
        def one(index, carry):
            group = around(index)

            def entry(j, state):
                count, picks = state
                for r in range(requests):
                    local = pages_ref[j, group * requests + r] - me * pool_pages
                    hit = jnp.where((local >= 0) & (local < pool_pages), 1, 0)
                    picks = tuple(
                        jnp.where((hit == 1) & (count == c), local, p) for c, p in enumerate(picks)
                    )
                    count = count + hit
                return count, picks

            zero = jnp.int32(0)
            _, picks = lax.fori_loop(
                0, pages_ref.shape[0], entry, (zero, (zero,) * prefix_cap), unroll=4
            )
            for c in range(prefix_cap):
                psend[index, c] = pool_ref[picks[c]]
            return carry

        lax.fori_loop(first, first + GROUPS_AT_ONCE, one, 0)

    def pick_source(first):
        def one(index, carry):
            group = around(index)

            def entry(e, state):
                count, picks = state
                hit = jnp.where(owner_ref[me * fresh_entries + e] == group, 1, 0)
                picks = tuple(
                    jnp.where((hit == 1) & (count == c), e, p) for c, p in enumerate(picks)
                )
                return count + hit, picks

            none = jnp.int32(fresh_entries)
            _, picks = lax.fori_loop(
                0, fresh_entries, entry, (jnp.int32(0), (none,) * fresh_cap), unroll=4
            )
            for c in range(fresh_cap):
                source[index * fresh_cap + c] = picks[c]
            return carry

        lax.fori_loop(first, first + GROUPS_AT_ONCE, one, 0)

    def finish_kv():
        for b in range(requests):
            mine = slice(b * BLOCK, (b + 1) * BLOCK)
            pair = acc[mine, :] + bkv_ref[...]
            key, value = pair[:, :HEAD_DIM], pair[:, HEAD_DIM:]
            at = pl.ds(plen_ref[me * requests + b], BLOCK)
            turned = key * cos_ref[at, :] + pltpu.roll(key, HEAD_DIM // 2, 1) * sin_ref[at, :]
            index = lax.broadcasted_iota(jnp.int32, (BLOCK, HEAD_DIM), 0)
            live = index < slen_ref[me * requests + b]
            key = jnp.where(live, turned, 0.0)
            value = jnp.where(live, value, 0.0)
            knew_ref[mine, :] = key.astype(jnp.bfloat16)
            vnew_ref[mine, :] = value.astype(jnp.bfloat16)
            count = BLOCK // PAGE
            pages = pl.ds(b * count, count)
            newp[pages, 0] = key.reshape(count, PAGE, HEAD_DIM).astype(jnp.bfloat16)
            newp[pages, 1] = value.reshape(count, PAGE, HEAD_DIM).astype(jnp.bfloat16)
        newp[fresh_entries] = jnp.zeros((2, PAGE, HEAD_DIM), jnp.bfloat16)

        def select(i, carry):
            for c in range(fresh_cap):
                fsend[i, c] = newp[source[i * fresh_cap + c]]
            return carry

        lax.fori_loop(0, n_seq, select, 0)
        fgot[me] = fsend[0]

    def fresh_copy(direction, step, behind):
        index = step if direction == 0 else n_r + step
        group = origin(1 - direction, step)
        there = me if not behind else origin(direction, step)
        return remote(
            fsend.at[index], fgot.at[there], fresh_send.at[index - 1], fresh_recv.at[index - 1],
            {"seq": group},
        )

    far_first = [
        (d, step) for step in range(n_r, 0, -1) for d in (0, 1) if step <= (n_r if d == 0 else n_l)
    ]

    work = []

    def fill(count):
        for _ in range(min(count, len(work))):
            work.pop(0)()

    work += [functools.partial(pick_pages, i) for i in range(0, n_seq, GROUPS_AT_ONCE)]
    sources = [functools.partial(pick_source, i) for i in range(0, n_seq, GROUPS_AT_ONCE)]
    products = []

    def compute(count):
        for _ in range(min(count, len(products))):
            product(*products.pop(0))

    wait = y_max + 1 if y_max else 0
    kv_end = n_r + Z_LAG[0] + Y_WAIT[0] + wait
    last = max(max(n_r + z + y + wait for z, y in zip(Z_LAG, Y_WAIT)), n_r + PREFIX_LAG)
    ready = 7
    for it in range(1, last + 1):
        busy = compute if it > ready else fill
        for w in range(2):
            step = it - Z_LAG[w]
            if step == 0:
                for d in (0, 1):
                    weights[w][d].start(1)
            if 1 <= step <= n_r:
                for d in (0, 1):
                    weights[w][d].arrive(step)
                    weights[w][d].start(step + 1)
            step -= Y_WAIT[w]
            if 1 <= step <= n_r:
                for d in (0, 1):
                    y_start(w, step, d, 1)
            busy(2)
        step = it - PREFIX_LAG
        if step == 0:
            fill(len(work))
            got_ref[0] = psend[0]
            for d in (0, 1):
                prefix[d].start(1)
            work += sources
        if 1 <= step <= n_r:
            for d in (0, 1):
                prefix[d].arrive(step)
                prefix[d].start(step + 1)
            got_ref[2 * step - 1] = pg_r[starts[0][step - 1]]
            if step <= n_l:
                got_ref[2 * step] = pg_l[starts[1][step - 1]]
        busy(1)
        for w in range(2):
            for hop in range(1, y_max + 1):
                step = it - Z_LAG[w] - Y_WAIT[w] - hop - 1
                if 1 <= step <= n_r:
                    for d in (0, 1):
                        y_arrive(w, step, d, hop)
                        y_start(w, step, d, hop + 1)
            step = it - Z_LAG[w] - Y_WAIT[w] - wait
            if 0 <= step <= n_r:
                products.append((w, step))
        if it == 3:
            tokens_near()
        if it == ready - 2:
            tokens_far()
        if it == ready - 1:
            tokens_here()
            normalise(0, half)
        if it == ready:
            normalise(half, half)
        if it > ready:
            fill(1)
        if it == kv_end:
            fill(len(work))
            products.sort(key=lambda item: item[0])
            compute(len([item for item in products if item[0] == 0]))
            finish_kv()
            for d, step in far_first:
                copy = fresh_copy(d, step, False)
                copy.start()
                opened.append(copy)
    compute(len(products))
    assert done == [n_r + 1] * 2 and not work

    for d, step in far_first:
        fresh_copy(d, step, True).wait_recv()
    fresh_ref[...] = fgot[...]
    for pair in [*weights, prefix]:
        for one in pair:
            one.drain()
    for copy in [*y_open.values(), *opened]:
        copy.wait_send()


def attend_kernel(
    n_seq, pool_pages,
    q_ref, bq_ref, cos_ref, sin_ref, knew_ref, vnew_ref, got_ref,
    pages_ref, plen_ref, slen_ref,
    out_ref, kall, vall, counts,
):
    me = lax.axis_index("seq")
    rows = q_ref.shape[0]
    requests = rows // BLOCK
    slots = pages_ref.shape[0]
    old = slots * PAGE
    heads = q_ref.shape[1] // HEAD_DIM
    cap = got_ref.shape[0] // n_seq
    n_r = n_seq // 2

    def clear(i, carry):
        counts[i] = 0
        return carry

    lax.fori_loop(0, n_seq, clear, 0)

    def page(j, carry):
        to = pl.ds(pl.multiple_of(j * PAGE, PAGE), PAGE)
        for b in range(requests):
            owner = lax.div(pages_ref[j, me * requests + b], pool_pages)
            rank = counts[owner]
            counts[owner] = rank + 1
            away = me - owner
            away = jnp.where(away < 0, away + n_seq, away)
            place = jnp.where(away <= n_r, 2 * away - 1, 2 * (n_seq - away))
            place = jnp.where(away == 0, 0, place)
            index = place * cap + rank
            kall[b, to, :] = got_ref[index, 0].astype(jnp.float32)
            vall[b, to, :] = got_ref[index, 1].astype(jnp.float32)
        return carry

    lax.fori_loop(0, slots, page, 0, unroll=4)
    for b in range(requests):
        mine = slice(b * BLOCK, (b + 1) * BLOCK)
        kall[b, old:, :] = knew_ref[mine, :].astype(jnp.float32)
        vall[b, old:, :] = vnew_ref[mine, :].astype(jnp.float32)
        keys = kall[b].astype(jnp.bfloat16)
        values = vall[b].astype(jnp.bfloat16)
        here = me * requests + b
        key_pos = lax.broadcasted_iota(jnp.int32, (BLOCK, old + BLOCK), 1)
        query_pos = lax.broadcasted_iota(jnp.int32, (BLOCK, old + BLOCK), 0)
        shifted = key_pos - old
        allowed = ((shifted < 0) & (key_pos < plen_ref[here])) | (
            (shifted >= 0) & (shifted <= query_pos) & (shifted < slen_ref[here])
        )
        live = lax.broadcasted_iota(jnp.int32, (BLOCK, HEAD_DIM), 0) < slen_ref[here]
        at = pl.ds(plen_ref[here], BLOCK)
        cos, sin = cos_ref[at, :], sin_ref[at, :]
        for h in range(heads):
            lin = q_ref[mine, h * HEAD_DIM : (h + 1) * HEAD_DIM]
            lin = lin + bq_ref[:, h * HEAD_DIM : (h + 1) * HEAD_DIM]
            query = (lin * cos + pltpu.roll(lin, HEAD_DIM // 2, 1) * sin).astype(jnp.bfloat16)
            scores = lax.dot_general(
                query, keys, (((1,), (1,)), ((), ())), preferred_element_type=jnp.float32
            ) * (1.0 / math.sqrt(HEAD_DIM))
            masked = jnp.where(allowed, scores, -1e30)
            peak = jnp.max(masked, axis=1, keepdims=True)
            weights = jnp.where(allowed, jnp.exp(masked - peak), 0.0)
            probs = (weights * (1.0 / jnp.sum(weights, axis=1, keepdims=True))).astype(jnp.bfloat16)
            mixed = jnp.dot(probs, values, preferred_element_type=jnp.float32)
            out_ref[mine, h * HEAD_DIM : (h + 1) * HEAD_DIM] = jnp.where(live, mixed, 0.0).astype(
                jnp.bfloat16
            )


def body(
    n_parts,
    tokens, norm_gain, w_query, w_kv, b_query, b_kv, kv_pool, prefix_pages, prefix_len, suffix_len,
    fresh_owner,
):
    n_seq, n_tp = lax.axis_size("seq"), lax.axis_size("tp")
    rows, features = tokens.shape
    requests = rows // BLOCK
    depth, query_width = w_query.shape
    kv_width = w_kv.shape[2]
    pool_pages = kv_pool.shape[0]
    slots = prefix_pages.shape[1]
    entries = requests * slots
    fresh_entries = rows // PAGE
    prefix_cap = max(3, entries // n_seq + 1)
    fresh_cap = max(2, (fresh_entries + n_seq - 1) // n_seq + 1)
    n_r, n_l = n_seq // 2, (n_seq - 1) // 2

    half_dim = HEAD_DIM // 2
    positions = np.arange(slots * PAGE + BLOCK, dtype=np.float32)[:, None]
    inverse = np.exp(
        np.arange(half_dim, dtype=np.float32) * np.float32(-2.0 * math.log(1000000.0) / HEAD_DIM)
    )
    angles = positions * inverse
    cosine, sine = np.cos(angles), np.sin(angles)
    cos_all = jnp.asarray(np.concatenate([cosine, cosine], axis=1), jnp.float32)
    sin_all = jnp.asarray(np.concatenate([-sine, sine], axis=1), jnp.float32)
    pages_by_slot = prefix_pages.T

    piece = depth // n_parts
    y_lanes = max(1, n_parts - 1)
    tri_r, tri_l = offsets(n_r)[1], offsets(n_l)[1]
    page = (2, PAGE, HEAD_DIM)
    bf16, f32 = jnp.bfloat16, jnp.float32
    vmem = pl.BlockSpec(memory_space=pltpu.VMEM)
    smem = pl.BlockSpec(memory_space=pltpu.SMEM)
    dma = pltpu.SemaphoreType.DMA
    q_sums, knew, vnew, got, fresh = pl.pallas_call(
        functools.partial(gather_kernel, n_parts, n_seq, n_tp),
        name="gather",
        out_shape=(
            jax.ShapeDtypeStruct((rows, query_width), f32),
            jax.ShapeDtypeStruct((rows, HEAD_DIM), bf16),
            jax.ShapeDtypeStruct((rows, HEAD_DIM), bf16),
            jax.ShapeDtypeStruct((n_seq, prefix_cap, *page), bf16),
            jax.ShapeDtypeStruct((n_seq, fresh_cap, *page), bf16),
        ),
        in_specs=[vmem] * 8 + [smem] * 4,
        out_specs=(vmem,) * 5,
        scratch_shapes=[
            pltpu.VMEM((n_tp, rows, features), bf16),
            pltpu.VMEM((n_tp, 1, features), f32),
            pltpu.VMEM((n_seq, rows, depth), bf16),
            pltpu.VMEM((n_seq, n_parts, piece, 2 * kv_width), bf16),
            pltpu.VMEM((n_seq, n_parts, piece, query_width), bf16),
            pltpu.VMEM((rows, 2 * kv_width), f32),
            pltpu.VMEM((n_seq, prefix_cap, *page), bf16),
            pltpu.VMEM((tri_r, prefix_cap, *page), bf16),
            pltpu.VMEM((tri_l, prefix_cap, *page), bf16),
            pltpu.VMEM((n_seq, fresh_cap, *page), bf16),
            pltpu.VMEM((n_seq, fresh_cap, *page), bf16),
            pltpu.VMEM((fresh_entries + 1, *page), bf16),
            pltpu.SMEM((n_seq * fresh_cap,), jnp.int32),
            dma((3, 2, 2)),
            dma((3, 2, n_r)),
            dma((2, y_lanes, 2)),
            dma((2, y_lanes, n_r)),
            dma((9,)),
            dma((9,)),
            dma((n_tp - 1,)),
            dma((n_tp - 1,)),
            dma((n_seq - 1,)),
            dma((n_seq - 1,)),
        ],
        compiler_params=pltpu.CompilerParams(
            collective_id=0, has_side_effects=True, vmem_limit_bytes=60 * 1024 * 1024
        ),
    )(
        tokens,
        norm_gain.astype(f32).reshape(1, features),
        w_kv.reshape(n_parts, piece, 2 * kv_width),
        w_query.reshape(n_parts, piece, query_width),
        b_kv.reshape(1, 2 * kv_width),
        cos_all,
        sin_all,
        kv_pool,
        pages_by_slot,
        prefix_len,
        suffix_len,
        fresh_owner.reshape(-1),
    )
    attn_out = pl.pallas_call(
        functools.partial(attend_kernel, n_seq, pool_pages),
        name="attend",
        out_shape=jax.ShapeDtypeStruct((rows, query_width), bf16),
        in_specs=[vmem] * 7 + [smem] * 3,
        out_specs=vmem,
        scratch_shapes=[
            pltpu.VMEM((requests, slots * PAGE + BLOCK, HEAD_DIM), f32),
            pltpu.VMEM((requests, slots * PAGE + BLOCK, HEAD_DIM), f32),
            pltpu.SMEM((n_seq,), jnp.int32),
        ],
    )(
        q_sums,
        b_query.reshape(1, query_width),
        cos_all,
        sin_all,
        knew,
        vnew,
        got.reshape(n_seq * prefix_cap, *page),
        pages_by_slot,
        prefix_len,
        suffix_len,
    )
    return attn_out, fresh.reshape(n_seq * fresh_cap, *page)


def solution(mesh):
    placed = (
        P(("parts", "seq"), "tp"),
        P("tp"),
        P("seq", "tp"),
        P("seq", None, "tp"),
        P("tp"),
        P(None, "tp"),
        P(("parts", "seq"), None, None, "tp"),
        P("parts", None),
        P("parts"),
        P("parts"),
        P("parts", None),
    )
    return jax.shard_map(
        functools.partial(body, mesh.shape["parts"]),
        mesh=mesh,
        in_specs=placed,
        out_specs=(P(("parts", "seq"), "tp"), P(("parts", "seq"), None, None, "tp")),
        check_vma=False,
    )
```
